16 devices in a mesh: depth: 2 (over z), col: 2 (over y), row: 4 (over x, core).
Axes of the slice: x: 2, y: 2, z: 2, core: 2. Of those that a mesh axis runs over, the one named last changes fastest.
Arguments:
- a_mat: bfloat16 [3072, 3072], P(('row', 'depth'), 'col')
- b_mat: bfloat16 [3072, 3072], P(('row', 'depth'), 'col')
Outputs:
- output: bfloat16 [3072, 3072], P(('row', 'depth'), 'col')
All inputs are finite; a program needn't handle non-finite values.
Results may differ from the reference program's by a relative error of at most 0.001.
Values are sent between devices in bfloat16 or wider.
A program may use at most 1 GiB of HBM per device.

```python
import jax
import jax.numpy as jnp

N = 3072


def setup_inputs(seed: int = 0) -> dict:
    key_a, key_b = jax.random.split(jax.random.key(seed))
    unit_scale = N ** -0.25
    a_vals = jax.random.normal(key_a, (N, N), jnp.float32) + unit_scale
    b_vals = jax.random.normal(key_b, (N, N), jnp.float32) + unit_scale
    a_mat = (a_vals * unit_scale).astype(jnp.bfloat16)
    b_mat = (b_vals * unit_scale).astype(jnp.bfloat16)
    return {"a_mat": a_mat, "b_mat": b_mat}


def reference(a_mat, b_mat):
    return jnp.dot(a_mat, b_mat, preferred_element_type=jnp.float32).astype(jnp.bfloat16)
```

```python
import functools

import jax
import jax.numpy as jnp
from jax import lax
from jax.experimental import pallas as pl
from jax.experimental.pallas import tpu as pltpu
from jax.sharding import PartitionSpec as P

MESH = pl.DeviceIdType.MESH
BLOCKS = 6


def kernel(blocks, a_hbm, b_hbm, c_ref, a_buf, b_buf, total,
           a_in, b_in, xs, xr, zs, zr, ys, yr, fxs, fxr, fzs, fzr,
           pos, por, pxs, pxr, pzs, pzr, pas, par, pbs, pbr):
    z = lax.axis_index("depth")
    y = lax.axis_index("col")
    row = lax.axis_index("row")
    x = row // 2
    c = row % 2
    ox, oy, oz = 1 - x, 1 - y, 1 - z
    rows, width = b_buf.shape[4], b_buf.shape[5]
    half = rows // 2
    partner = (z, y, 2 * x + 1 - c)
    x_dev = (z, y, 2 * ox + c)
    y_dev = (z, oy, row)
    z_dev = (oz, y, row)
    lo, hi = pl.ds(0, half), pl.ds(half, half)

    def remote(src, dst, send, recv, dev):
        return pltpu.make_async_remote_copy(
            src_ref=src, dst_ref=dst, send_sem=send, recv_sem=recv,
            device_id=dev, device_id_type=MESH)

    def same(ref, send, recv, dev):
        return remote(ref, ref, send, recv, dev)

    b_loads = [pltpu.make_async_copy(
        b_hbm.at[:, pl.ds(b * width, width)], b_buf.at[x, z, b, c], b_in.at[b]) for b in range(blocks)]
    a_loads = [pltpu.make_async_copy(
        a_hbm.at[:, pl.ds(q * rows, rows)], a_buf.at[y, q % 2, q // 2], a_in.at[q]) for q in range(4)]
    for load in b_loads + a_loads:
        load.start()

    barrier = pltpu.get_barrier_semaphore()
    for dev in (partner, x_dev, y_dev, z_dev):
        pl.semaphore_signal(barrier, inc=1, device_id=dev, device_id_type=MESH)
    pl.semaphore_wait(barrier, 4)

    sends = []

    def go(copy):
        copy.start()
        sends.append(copy)

    for b in range(blocks):
        b_loads[b].wait()
        go(same(b_buf.at[x, z, b, c], xs.at[b], xr.at[b], x_dev))
        go(same(b_buf.at[x, z, b, c], zs.at[b], zr.at[b], z_dev))
        if b == 0:
            for load in a_loads:
                load.wait()
            go(same(a_buf.at[y], ys, yr, y_dev))
        go(same(b_buf.at[x, z, b, c], pos.at[b], por.at[b], partner))

    for b in range(blocks):
        same(b_buf.at[x, oz, b, c], zs.at[b], zr.at[b], z_dev).wait_recv()
        go(same(b_buf.at[x, oz, b, c, lo], fxs.at[b], fxr.at[b], x_dev))
        go(same(b_buf.at[x, oz, b, c], pzs.at[b], pzr.at[b], partner))
        same(b_buf.at[ox, z, b, c], xs.at[b], xr.at[b], x_dev).wait_recv()
        go(same(b_buf.at[ox, z, b, c, hi], fzs.at[b], fzr.at[b], z_dev))
        go(same(b_buf.at[ox, z, b, c], pxs.at[b], pxr.at[b], partner))

    same(a_buf.at[oy], ys, yr, y_dev).wait_recv()
    for b in range(blocks):
        same(b_buf.at[x, z, b, 1 - c], pos.at[b], por.at[b], partner).wait_recv()
        same(b_buf.at[x, oz, b, 1 - c], pzs.at[b], pzr.at[b], partner).wait_recv()
        same(b_buf.at[ox, z, b, 1 - c], pxs.at[b], pxr.at[b], partner).wait_recv()

    def product(xk, zk, b):
        lhs = jnp.concatenate([a_buf[xk, zk, 0], a_buf[xk, zk, 1]], axis=1)
        rhs = b_buf[xk, zk, b].reshape(2 * rows, width)
        return jnp.dot(lhs, rhs, preferred_element_type=jnp.float32)

    @pl.loop(0, blocks)
    def _(b):
        total[b] = product(x, z, b) + product(x, oz, b) + product(ox, z, b)

    for b in range(blocks):
        same(b_buf.at[ox, oz, b, c, lo], fxs.at[b], fxr.at[b], x_dev).wait_recv()
        go(same(b_buf.at[ox, oz, b, c, lo], pas.at[b], par.at[b], partner))
        same(b_buf.at[ox, oz, b, c, hi], fzs.at[b], fzr.at[b], z_dev).wait_recv()
        go(same(b_buf.at[ox, oz, b, c, hi], pbs.at[b], pbr.at[b], partner))
        same(b_buf.at[ox, oz, b, 1 - c, lo], pas.at[b], par.at[b], partner).wait_recv()
        same(b_buf.at[ox, oz, b, 1 - c, hi], pbs.at[b], pbr.at[b], partner).wait_recv()
        c_ref[:, pl.ds(b * width, width)] = (total[b] + product(ox, oz, b)).astype(c_ref.dtype)

    for copy in sends:
        copy.wait_send()


def solution(mesh):
    def local_product(a_blk, b_blk):
        rows, cols = a_blk.shape
        width = cols // BLOCKS
        dma = pltpu.SemaphoreType.DMA
        per_block = [dma((BLOCKS,))] * 2
        return pl.pallas_call(
            functools.partial(kernel, BLOCKS),
            out_shape=jax.ShapeDtypeStruct((rows, cols), jnp.bfloat16),
            in_specs=[pl.BlockSpec(memory_space=pl.ANY)] * 2,
            out_specs=pl.BlockSpec(memory_space=pltpu.VMEM),
            scratch_shapes=[
                pltpu.VMEM((2, 2, 2, rows, rows), jnp.bfloat16),
                pltpu.VMEM((2, 2, BLOCKS, 2, rows, width), jnp.bfloat16),
                pltpu.VMEM((BLOCKS, rows, width), jnp.float32),
                dma((4,)), dma((BLOCKS,)),
                *per_block, *per_block, dma, dma, *per_block, *per_block,
                *per_block, *per_block, *per_block, *per_block, *per_block,
            ],
            compiler_params=pltpu.CompilerParams(collective_id=0, has_side_effects=True),
        )(a_blk, b_blk)

    block_spec = P(("row", "depth"), "col")
    return jax.shard_map(local_product, mesh=mesh, in_specs=(block_spec, block_spec), out_specs=block_spec, check_vma=False)
```

```python
import functools

import jax
import jax.numpy as jnp
from jax import lax
from jax.experimental import pallas as pl
from jax.experimental.pallas import tpu as pltpu
from jax.sharding import PartitionSpec as P

MESH = pl.DeviceIdType.MESH
BLOCKS = 3


def kernel(blocks, a_hbm, b_hbm, c_ref, a_buf, b_buf, total,
           a_in, b_in, xs, xr, zs, zr, ys, yr, fxs, fxr, fzs, fzr,
           pos, por, pxs, pxr, pzs, pzr, pas, par, pbs, pbr):
    z = lax.axis_index("depth")
    y = lax.axis_index("col")
    row = lax.axis_index("row")
    x = row // 2
    c = row % 2
    ox, oy, oz = 1 - x, 1 - y, 1 - z
    rows, width = b_buf.shape[4], b_buf.shape[5]
    half = rows // 2
    partner = (z, y, 2 * x + 1 - c)
    x_dev = (z, y, 2 * ox + c)
    y_dev = (z, oy, row)
    z_dev = (oz, y, row)
    lo, hi = pl.ds(0, half), pl.ds(half, half)

    def remote(src, dst, send, recv, dev):
        return pltpu.make_async_remote_copy(
            src_ref=src, dst_ref=dst, send_sem=send, recv_sem=recv,
            device_id=dev, device_id_type=MESH)

    def same(ref, send, recv, dev):
        return remote(ref, ref, send, recv, dev)

    b_loads = [pltpu.make_async_copy(
        b_hbm.at[:, pl.ds(b * width, width)], b_buf.at[x, z, b, c], b_in.at[b]) for b in range(blocks)]
    a_loads = [pltpu.make_async_copy(
        a_hbm.at[:, pl.ds(q * rows, rows)], a_buf.at[y, q % 2, q // 2], a_in.at[q]) for q in range(4)]
    for load in b_loads + a_loads:
        load.start()

    barrier = pltpu.get_barrier_semaphore()
    for dev in (partner, x_dev, y_dev, z_dev):
        pl.semaphore_signal(barrier, inc=1, device_id=dev, device_id_type=MESH)
    pl.semaphore_wait(barrier, 4)

    sends = []

    def go(copy):
        copy.start()
        sends.append(copy)

    for b in range(blocks):
        b_loads[b].wait()
        go(same(b_buf.at[x, z, b, c], xs.at[b], xr.at[b], x_dev))
        go(same(b_buf.at[x, z, b, c], zs.at[b], zr.at[b], z_dev))
        if b == 0:
            for load in a_loads:
                load.wait()
            go(same(a_buf.at[y], ys, yr, y_dev))
        go(same(b_buf.at[x, z, b, c], pos.at[b], por.at[b], partner))

    for b in range(blocks):
        same(b_buf.at[x, oz, b, c], zs.at[b], zr.at[b], z_dev).wait_recv()
        go(same(b_buf.at[x, oz, b, c, lo], fxs.at[b], fxr.at[b], x_dev))
        go(same(b_buf.at[x, oz, b, c], pzs.at[b], pzr.at[b], partner))
        same(b_buf.at[ox, z, b, c], xs.at[b], xr.at[b], x_dev).wait_recv()
        go(same(b_buf.at[ox, z, b, c, hi], fzs.at[b], fzr.at[b], z_dev))
        go(same(b_buf.at[ox, z, b, c], pxs.at[b], pxr.at[b], partner))

    same(a_buf.at[oy], ys, yr, y_dev).wait_recv()
    for b in range(blocks):
        same(b_buf.at[x, z, b, 1 - c], pos.at[b], por.at[b], partner).wait_recv()
        same(b_buf.at[x, oz, b, 1 - c], pzs.at[b], pzr.at[b], partner).wait_recv()
        same(b_buf.at[ox, z, b, 1 - c], pxs.at[b], pxr.at[b], partner).wait_recv()

    def product(xk, zk, b):
        lhs = jnp.concatenate([a_buf[xk, zk, 0], a_buf[xk, zk, 1]], axis=1)
        rhs = b_buf[xk, zk, b].reshape(2 * rows, width)
        return jnp.dot(lhs, rhs, preferred_element_type=jnp.float32)

    @pl.loop(0, blocks)
    def _(b):
        total[b] = product(x, z, b) + product(x, oz, b) + product(ox, z, b)

    for b in range(blocks):
        same(b_buf.at[ox, oz, b, c, lo], fxs.at[b], fxr.at[b], x_dev).wait_recv()
        go(same(b_buf.at[ox, oz, b, c, lo], pas.at[b], par.at[b], partner))
        same(b_buf.at[ox, oz, b, c, hi], fzs.at[b], fzr.at[b], z_dev).wait_recv()
        go(same(b_buf.at[ox, oz, b, c, hi], pbs.at[b], pbr.at[b], partner))
        same(b_buf.at[ox, oz, b, 1 - c, lo], pas.at[b], par.at[b], partner).wait_recv()
        same(b_buf.at[ox, oz, b, 1 - c, hi], pbs.at[b], pbr.at[b], partner).wait_recv()
        c_ref[:, pl.ds(b * width, width)] = (total[b] + product(ox, oz, b)).astype(c_ref.dtype)

    for copy in sends:
        copy.wait_send()


def solution(mesh):
    def local_product(a_blk, b_blk):
        rows, cols = a_blk.shape
        width = cols // BLOCKS
        dma = pltpu.SemaphoreType.DMA
        per_block = [dma((BLOCKS,))] * 2
        return pl.pallas_call(
            functools.partial(kernel, BLOCKS),
            out_shape=jax.ShapeDtypeStruct((rows, cols), jnp.bfloat16),
            in_specs=[pl.BlockSpec(memory_space=pl.ANY)] * 2,
            out_specs=pl.BlockSpec(memory_space=pltpu.VMEM),
            scratch_shapes=[
                pltpu.VMEM((2, 2, 2, rows, rows), jnp.bfloat16),
                pltpu.VMEM((2, 2, BLOCKS, 2, rows, width), jnp.bfloat16),
                pltpu.VMEM((BLOCKS, rows, width), jnp.float32),
                dma((4,)), dma((BLOCKS,)),
                *per_block, *per_block, dma, dma, *per_block, *per_block,
                *per_block, *per_block, *per_block, *per_block, *per_block,
            ],
            compiler_params=pltpu.CompilerParams(collective_id=0, has_side_effects=True),
        )(a_blk, b_blk)

    block_spec = P(("row", "depth"), "col")
    return jax.shard_map(local_product, mesh=mesh, in_specs=(block_spec, block_spec), out_specs=block_spec, check_vma=False)
```

```python
import functools

import jax
import jax.numpy as jnp
from jax import lax
from jax.experimental import pallas as pl
from jax.experimental.pallas import tpu as pltpu
from jax.sharding import PartitionSpec as P

MESH = pl.DeviceIdType.MESH
BLOCKS = 3


def kernel(blocks, a_hbm, b_hbm, c_ref, a_buf, b_buf, total,
           a_in, b_in, xs, xr, zs, zr, ys, yr, fxs, fxr, fzs, fzr,
           pos, por, pxs, pxr, pzs, pzr, pas, par, pbs, pbr):
    z = lax.axis_index("depth")
    y = lax.axis_index("col")
    row = lax.axis_index("row")
    x = row // 2
    c = row % 2
    ox, oy, oz = 1 - x, 1 - y, 1 - z
    rows, width = b_buf.shape[4], b_buf.shape[5]
    half = rows // 2
    partner = (z, y, 2 * x + 1 - c)
    x_dev = (z, y, 2 * ox + c)
    y_dev = (z, oy, row)
    z_dev = (oz, y, row)
    lo, hi = pl.ds(0, half), pl.ds(half, half)

    def remote(src, dst, send, recv, dev):
        return pltpu.make_async_remote_copy(
            src_ref=src, dst_ref=dst, send_sem=send, recv_sem=recv,
            device_id=dev, device_id_type=MESH)

    def same(ref, send, recv, dev):
        return remote(ref, ref, send, recv, dev)

    b_loads = [pltpu.make_async_copy(
        b_hbm.at[:, pl.ds(b * width, width)], b_buf.at[x, z, b, c], b_in.at[b]) for b in range(blocks)]
    a_loads = [pltpu.make_async_copy(
        a_hbm.at[:, pl.ds(q * rows, rows)], a_buf.at[y, q % 2, q // 2], a_in.at[q]) for q in range(4)]
    for load in b_loads + a_loads:
        load.start()

    barrier = pltpu.get_barrier_semaphore()
    for dev in (partner, x_dev, y_dev, z_dev):
        pl.semaphore_signal(barrier, inc=1, device_id=dev, device_id_type=MESH)
    pl.semaphore_wait(barrier, 4)

    sends = []

    def go(copy):
        copy.start()
        sends.append(copy)

    for b in range(blocks):
        b_loads[b].wait()
        go(same(b_buf.at[x, z, b, c], xs.at[b], xr.at[b], x_dev))
        go(same(b_buf.at[x, z, b, c], zs.at[b], zr.at[b], z_dev))
        if b == 0:
            for load in a_loads:
                load.wait()
            go(same(a_buf.at[y], ys, yr, y_dev))
        go(same(b_buf.at[x, z, b, c], pos.at[b], por.at[b], partner))

    for b in range(blocks):
        same(b_buf.at[x, oz, b, c], zs.at[b], zr.at[b], z_dev).wait_recv()
        go(same(b_buf.at[x, oz, b, c, lo], fxs.at[b], fxr.at[b], x_dev))
        go(same(b_buf.at[x, oz, b, c], pzs.at[b], pzr.at[b], partner))
        same(b_buf.at[ox, z, b, c], xs.at[b], xr.at[b], x_dev).wait_recv()
        go(same(b_buf.at[ox, z, b, c, hi], fzs.at[b], fzr.at[b], z_dev))
        go(same(b_buf.at[ox, z, b, c], pxs.at[b], pxr.at[b], partner))

    same(a_buf.at[oy], ys, yr, y_dev).wait_recv()
    for b in range(blocks):
        same(b_buf.at[x, z, b, 1 - c], pos.at[b], por.at[b], partner).wait_recv()
        same(b_buf.at[x, oz, b, 1 - c], pzs.at[b], pzr.at[b], partner).wait_recv()
        same(b_buf.at[ox, z, b, 1 - c], pxs.at[b], pxr.at[b], partner).wait_recv()

    def product(xk, zk, b):
        lhs = jnp.concatenate([a_buf[xk, zk, 0], a_buf[xk, zk, 1]], axis=1)
        rhs = b_buf[xk, zk, b].reshape(2 * rows, width)
        return jnp.dot(lhs, rhs, preferred_element_type=jnp.float32)

    @pl.loop(0, blocks)
    def _(b):
        total[b] = product(x, z, b) + product(x, oz, b) + product(ox, z, b)

    for b in range(blocks):
        same(b_buf.at[ox, oz, b, c, lo], fxs.at[b], fxr.at[b], x_dev).wait_recv()
        go(same(b_buf.at[ox, oz, b, c, lo], pas.at[b], par.at[b], partner))
        same(b_buf.at[ox, oz, b, c, hi], fzs.at[b], fzr.at[b], z_dev).wait_recv()
        go(same(b_buf.at[ox, oz, b, c, hi], pbs.at[b], pbr.at[b], partner))
        same(b_buf.at[ox, oz, b, 1 - c, lo], pas.at[b], par.at[b], partner).wait_recv()
        same(b_buf.at[ox, oz, b, 1 - c, hi], pbs.at[b], pbr.at[b], partner).wait_recv()
        c_ref[:, pl.ds(b * width, width)] = (total[b] + product(ox, oz, b)).astype(c_ref.dtype)

    for copy in sends:
        copy.wait_send()


def solution(mesh):
    def local_product(a_blk, b_blk):
        rows, cols = a_blk.shape
        width = cols // BLOCKS
        dma = pltpu.SemaphoreType.DMA
        per_block = [dma((BLOCKS,))] * 2
        return pl.pallas_call(
            functools.partial(kernel, BLOCKS),
            out_shape=pltpu.VMEM((rows, cols), jnp.bfloat16),
            in_specs=[pl.BlockSpec(memory_space=pl.ANY)] * 2,
            out_specs=pl.BlockSpec(memory_space=pltpu.VMEM),
            scratch_shapes=[
                pltpu.VMEM((2, 2, 2, rows, rows), jnp.bfloat16),
                pltpu.VMEM((2, 2, BLOCKS, 2, rows, width), jnp.bfloat16),
                pltpu.VMEM((BLOCKS, rows, width), jnp.float32),
                dma((4,)), dma((BLOCKS,)),
                *per_block, *per_block, dma, dma, *per_block, *per_block,
                *per_block, *per_block, *per_block, *per_block, *per_block,
            ],
            compiler_params=pltpu.CompilerParams(collective_id=0, has_side_effects=True),
        )(a_blk, b_blk)

    block_spec = P(("row", "depth"), "col")
    return jax.shard_map(local_product, mesh=mesh, in_specs=(block_spec, block_spec), out_specs=block_spec, check_vma=False)
```
